32 devices in a mesh: tm: 4 (over z), ent: 8 (over y, x, core).
Axes of the slice: x: 2, y: 2, z: 4, core: 2. Of those that a mesh axis runs over, the one named last changes fastest.
Arguments:
- states: bfloat16 [4, 8192, 512], P('tm', 'ent'), may hold values from -6 to 6
- cotangent: bfloat16 [4, 8192, 512], P('tm', 'ent'), may hold values from -6 to 6
- export_rows: int32 [4, 2048], P('tm', 'ent'), may hold values from 0 to 1023
- edge_src: int32 [4, 8192], P('tm', 'ent'), may hold values from 0 to 255
- edge_dst: int32 [4, 8192], P('tm', 'ent'), may hold values from 0 to 1023
- edge_rel: int32 [4, 8192], P('tm', 'ent'), may hold values from 0 to 255
- tile_count: int32 [4, 8], P('tm', 'ent'), may hold values from 1 to 8, as said below
- basis: bfloat16 [512, 2048], replicated, may hold values from -0.25 to 0.25
- coef: float32 [256, 4], replicated, may hold values from -3 to 3
- rel_emb: bfloat16 [256, 512], replicated, may hold values from -3 to 3
- self_weight: bfloat16 [512, 512], replicated, may hold values from -0.25 to 0.25
- gate_weight: bfloat16 [512, 512], replicated, may hold values from -0.25 to 0.25
- gate_bias: float32 [512], replicated, may hold values from -2 to 1
Outputs:
- grad_states: float32 [4, 8192, 512], P('tm', 'ent')
- grad_basis: float32 [512, 2048], P('ent')
- grad_self: float32 [512, 512], P('ent')
- grad_gate: float32 [512, 512], P('ent')
- grad_gate_bias: float32 [512], P('ent')
- grad_coef: float32 [256, 4], P('ent')
- grad_rel_emb: float32 [256, 512], P('ent')
The draws below stay inside these ranges and needn't reach their ends.
Inputs may be any that keep to these rules, and one draw needn't show every extreme that they name: `tile_count`: some slab of some snapshot has 8 live tiles in every draw.
All inputs are finite; a program needn't handle non-finite values.
Results may differ from the reference program's by a relative error of at most 0.01.
Values may be sent and summed in bfloat16 or wider, within the bound.
No kernel may reach another device: no remote copies, remote signals or barrier semaphores. Data moves between devices by JAX's collectives and lax.ppermute only.
A program may use at most 128 MiB of HBM per device.

```python
import math
import jax
import jax.numpy as jnp
import numpy as np

D = 512
NREL = 256
NB = 4
TILE = 128
ROWS_DEV = 1024
TILES = 8
CAP = 32
SNAPS = 4
ENTITIES = 8192
SLOTS = 256
EDGES_DEV = 1024
N_ENT = 8


def draw_tile_count(key, part):
    key_first = jax.random.fold_in(key, 11)
    key_second = jax.random.fold_in(key, 12)
    key_third = jax.random.fold_in(key, 13)
    first_draw = jax.random.randint(key_first, (SNAPS * N_ENT,), 1, TILES + 1)
    second_draw = jax.random.randint(key_second, (SNAPS * N_ENT,), 1, TILES + 1)
    flat_counts = jnp.minimum(first_draw, second_draw)
    full_place = jax.random.randint(key_third, (), 0, SNAPS * N_ENT)
    flat_counts = jnp.where(jnp.arange(SNAPS * N_ENT) == full_place, TILES, flat_counts)
    return flat_counts.reshape(SNAPS, N_ENT).astype(jnp.int32)


def plant(array, own_key, smallest, high):
    longest = array.shape.index(max(array.shape))
    spots = []
    for shift in (0, 1):
        where = [jax.random.randint(jax.random.fold_in(own_key, axis), (), 0, length) for axis, length in enumerate(array.shape)]
        where[longest] = (where[longest] + shift) % array.shape[longest]
        spots.append(tuple(where))
    return array.at[spots[0]].set(smallest).at[spots[1]].set(high)


def shard_levels(stream_key, shape, shards, smallest, high):
    def one(axis_at, blocks):
        steps = jax.random.uniform(jax.random.fold_in(jax.random.fold_in(stream_key, 6), axis_at), (blocks,), jnp.float32, smallest / len(shards), high / len(shards))
        return jnp.repeat(jnp.exp(steps), shape[axis_at] // blocks).reshape((-1,) + (1,) * (len(shape) - axis_at - 1))

    factor_of = one(*shards[0])
    for cut in shards[1:]:
        factor_of = factor_of * one(*cut)
    return factor_of


def rank_bounds(number_of, skew):
    portions = [(1 << 20) // math.isqrt(standing ** skew) + 1 for standing in range(1, number_of + 1)]
    spread = 1 + sum(portions) // (1 << 30)
    return np.cumsum(np.array([max(1, weight // spread) for weight in portions]))


def ranked_ids(key, shape, amount, skew):
    table = rank_bounds(amount, skew)
    ticket = jax.random.randint(jax.random.fold_in(key, 1), shape, 0, int(table[amount - 1]))
    standing = jnp.searchsorted(jnp.asarray(table, jnp.int32), ticket, side="right")
    return jax.random.permutation(jax.random.fold_in(key, 2), amount)[standing].astype(jnp.int32)


def gaussian(stream_key, extent, scale, limit, split=(), kind=jnp.bfloat16):
    entries = jax.random.normal(stream_key, extent, jnp.float32) * scale
    if len(split) > 0:
        entries = shard_levels(stream_key, extent, split, -0.22, 0.18) * entries
    return jnp.clip(entries, min=-limit, max=limit).astype(kind)


def setup_inputs(seed: int = 0) -> dict:
    streams_of = jax.random.split(jax.random.key(seed), 14)
    return {
        "states": gaussian(streams_of[0], (SNAPS, ENTITIES, D), 1.0, 6.0, ((0, 4), (1, 8))),
        "cotangent": gaussian(streams_of[1], (SNAPS, ENTITIES, D), 1.0, 6.0, ((0, 4), (1, 8))),
        "export_rows": plant(jax.random.randint(streams_of[2], (SNAPS, N_ENT * SLOTS), 0, ROWS_DEV), jax.random.fold_in(streams_of[2], 1), 0, ROWS_DEV - 1).astype(jnp.int32),
        "edge_src": plant(jax.random.randint(streams_of[3], (SNAPS, N_ENT * EDGES_DEV), 0, SLOTS), jax.random.fold_in(streams_of[3], 1), 0, SLOTS - 1).astype(jnp.int32),
        "edge_dst": plant(jax.random.randint(streams_of[4], (SNAPS, N_ENT * EDGES_DEV), 0, ROWS_DEV), jax.random.fold_in(streams_of[4], 1), 0, ROWS_DEV - 1).astype(jnp.int32),
        "edge_rel": plant(ranked_ids(streams_of[5], (SNAPS, N_ENT * EDGES_DEV), NREL, 2), jax.random.fold_in(streams_of[5], 3), 0, NREL - 1).astype(jnp.int32),
        "tile_count": draw_tile_count(jax.random.fold_in(streams_of[13], 71), 0),
        "basis": gaussian(streams_of[7], (D, NB * D), D ** -0.5, 0.25),
        "coef": gaussian(streams_of[8], (NREL, NB), 0.5, 3.0, (), jnp.float32),
        "rel_emb": gaussian(streams_of[9], (NREL, D), 0.5, 3.0),
        "self_weight": gaussian(streams_of[10], (D, D), D ** -0.5, 0.25),
        "gate_weight": gaussian(streams_of[11], (D, D), D ** -0.5, 0.25),
        "gate_bias": jnp.clip(jax.random.uniform(streams_of[12], (D,), jnp.float32, -2.0, 1.0), -2.0, 1.0),
    }


def reference(states, cotangent, export_rows, edge_src, edge_dst, edge_rel, tile_count, basis, coef, rel_emb, self_weight, gate_weight, gate_bias):
    edge_total = N_ENT * EDGES_DEV
    positions = jnp.arange(edge_total, dtype=jnp.int32)
    device_of = (positions // EDGES_DEV).astype(jnp.int32)
    handed = jnp.zeros((ENTITIES, D), jnp.bfloat16)
    basis_sum = jnp.zeros((D, NB * D), jnp.float32)
    self_sum = jnp.zeros((D, D), jnp.float32)
    gate_sum = jnp.zeros((D, D), jnp.float32)
    bias_sum = jnp.zeros((D,), jnp.float32)
    coef_sum = jnp.zeros((NREL, NB), jnp.float32)
    relation_sum = jnp.zeros((NREL, D), jnp.float32)
    grad_list = []
    for snapshot in range(SNAPS - 1, -1, -1):
        own_state = states[snapshot]
        owner = (edge_src[snapshot] // CAP).astype(jnp.int32)
        entry_slot = (edge_src[snapshot] % CAP).astype(jnp.int32)
        local_row = export_rows[snapshot][owner * (N_ENT * CAP) + device_of * CAP + entry_slot]
        source = (owner * ROWS_DEV + local_row).astype(jnp.int32)
        target = (device_of * ROWS_DEV + edge_dst[snapshot]).astype(jnp.int32)
        live_mask = ((positions % EDGES_DEV) // TILE) < tile_count[snapshot][device_of]
        relation = edge_rel[snapshot]
        edge_input = (own_state[source].astype(jnp.float32) + rel_emb[relation].astype(jnp.float32)).astype(jnp.bfloat16)
        images = jnp.dot(edge_input, basis, preferred_element_type=jnp.float32).reshape(edge_total, NB, D)
        edge_coef = coef[relation].astype(jnp.float32)
        message = jnp.einsum("eb,ebd->ed", edge_coef, images)
        message = jnp.where(live_mask[:, None], message, jnp.zeros((), jnp.float32))
        degree = 1.0 + jax.ops.segment_sum(live_mask.astype(jnp.float32), target, ENTITIES)
        self_part = jnp.dot(own_state, self_weight, preferred_element_type=jnp.float32)
        summed = (jax.ops.segment_sum(message, target, ENTITIES) + self_part) / degree[:, None]
        aggregated = jnp.tanh(summed)
        gate_open = jax.nn.sigmoid(jnp.dot(own_state, gate_weight, preferred_element_type=jnp.float32) + gate_bias)
        upstream = cotangent[snapshot].astype(jnp.float32) + handed.astype(jnp.float32)
        row_grad = (upstream * gate_open * (1.0 - aggregated * aggregated) / degree[:, None]).astype(jnp.bfloat16)
        gate_grad = upstream * (aggregated - own_state.astype(jnp.float32)) * gate_open * (1.0 - gate_open)
        gate_row = gate_grad.astype(jnp.bfloat16)
        edge_grad = jnp.where(live_mask[:, None], row_grad[target], jnp.zeros((), jnp.bfloat16))
        image_grad = (edge_coef[:, :, None] * edge_grad.astype(jnp.float32)[:, None, :]).astype(jnp.bfloat16).reshape(edge_total, NB * D)
        input_grad = jnp.dot(image_grad, basis.T, preferred_element_type=jnp.float32)
        state_grad = upstream * (1.0 - gate_open)
        state_grad = state_grad + jnp.dot(row_grad, self_weight.T, preferred_element_type=jnp.float32)
        state_grad = state_grad + jnp.dot(gate_row, gate_weight.T, preferred_element_type=jnp.float32)
        state_grad = state_grad + jax.ops.segment_sum(input_grad, source, ENTITIES)
        grad_list.append(state_grad)
        handed = state_grad.astype(jnp.bfloat16)
        basis_sum = basis_sum + jnp.dot(edge_input.T, image_grad, preferred_element_type=jnp.float32)
        self_sum = self_sum + jnp.dot(own_state.T, row_grad, preferred_element_type=jnp.float32)
        gate_sum = gate_sum + jnp.dot(own_state.T, gate_row, preferred_element_type=jnp.float32)
        bias_sum = bias_sum + jnp.sum(gate_grad, axis=0)
        coef_edge = jnp.einsum("ed,ebd->eb", edge_grad.astype(jnp.float32), images)
        coef_sum = coef_sum + jax.ops.segment_sum(coef_edge, relation, NREL)
        relation_sum = relation_sum + jax.ops.segment_sum(input_grad, relation, NREL)
    grad_states = jnp.stack(grad_list[::-1], axis=0)
    return (grad_states, basis_sum, self_sum, gate_sum, bias_sum, coef_sum, relation_sum)
```

```python
import functools

import jax
import jax.numpy as jnp
from jax import lax
from jax.experimental import pallas as pl
from jax.experimental.pallas import tpu as pltpu
from jax.sharding import PartitionSpec as P

TILE = 128
LANES = 128
BF = jnp.bfloat16
F32 = jnp.float32
VM = pltpu.VMEM


def dot(left, right, left_dim=1, right_dim=0):
    return lax.dot_general(
        left, right, (((left_dim,), (right_dim,)), ((), ())), preferred_element_type=F32
    )


def ones_where(mask):
    return jnp.where(mask, jnp.float32(1), jnp.float32(0)).astype(BF)


def rounded_up(value, unit):
    return -(-value // unit) * unit


def spread_column(row):
    return jnp.transpose(jnp.broadcast_to(row, (LANES, row.shape[1])))


def lane_tiled(column, lanes):
    return jnp.concatenate([column] * (lanes // LANES), axis=1)


def call(kernel, out_shape, args, scratch=(), smem=0, flops=0, limit=40 << 20):
    specs = [pl.BlockSpec(memory_space=pltpu.SMEM)] * smem
    specs += [pl.BlockSpec(memory_space=VM)] * (len(args) - smem)
    return pl.pallas_call(
        kernel,
        out_shape=out_shape,
        in_specs=specs,
        out_specs=jax.tree.map(lambda _: pl.BlockSpec(memory_space=VM), out_shape),
        scratch_shapes=list(scratch),
        compiler_params=pltpu.CompilerParams(vmem_limit_bytes=limit),
        cost_estimate=pl.CostEstimate(
            flops=flops, bytes_accessed=4 << 20, transcendentals=0
        ),
    )(*args)


def shape(dims, kind):
    return jax.ShapeDtypeStruct(dims, kind)


def tiles(total, size):
    size = min(total, size)

    def loop(body):
        def step(i, _):
            body(pl.ds(pl.multiple_of(i * size, size), size), i)
            return 0

        lax.fori_loop(0, total // size, step, 0)

    return loop


def export_kernel(states, export_row, sent):
    rows = states.shape[0]
    slots = export_row.shape[1]
    size = min(256, slots)

    @tiles(slots, size)
    def _(block, i):
        column = lane_tiled(spread_column(export_row[:, block]), rows)
        hot = ones_where(column == lax.broadcasted_iota(jnp.int32, (size, rows), 1))
        sent[block, :] = dot(hot, states[...]).astype(BF)


def setup_kernel(
    slots,
    tile_count,
    src_row,
    dst_row,
    rel_row,
    coef,
    coef_t,
    rel_emb,
    basis,
    states,
    self_weight,
    gate_weight,
    gate_bias,
    mix,
    counts,
    degree_inv,
    partial,
    gate,
    target,
    edge_coef,
    rel_images,
):
    rows, width = states.shape
    edges = src_row.shape[1]
    relations, blocks = coef.shape
    live_edges = tile_count[0, 0] * TILE
    size = 256

    @tiles(edges, size)
    def _(block, i):
        column = lane_tiled(spread_column(dst_row[:, block]), rows)
        edge = lax.broadcasted_iota(jnp.int32, (size, rows), 0) + i * size
        row = lax.broadcasted_iota(jnp.int32, (size, rows), 1)
        target[block, :] = ones_where((column == row) & (edge < live_edges))

    rel_hot = ones_where(
        rel_row[...] == lax.broadcasted_iota(jnp.int32, (relations, edges), 0)
    )
    edge_coef[...] = dot(coef_t[...].astype(BF), rel_hot)
    counts[...] = dot(rel_hot, target[...]).astype(BF)
    degree = 1.0 + dot(jnp.ones((8, edges), BF), target[...])
    degree_inv[...] = spread_column((1.0 / degree)[:1])
    part = min(256, slots)
    for b in range(blocks):

        @tiles(slots, part)
        def _(block, i):
            slot = lax.broadcasted_iota(jnp.int32, (part, edges), 0) + i * part
            weighted = jnp.where(
                src_row[...] == slot,
                jnp.broadcast_to(edge_coef[b : b + 1, :], (part, edges)),
                jnp.float32(0),
            ).astype(BF)
            mix[pl.ds(pl.multiple_of(b * slots + i * part, part), part), :] = dot(
                weighted, target[...]
            ).astype(BF)

    folded = jnp.zeros((relations, width), F32)
    for b in range(blocks):
        folded += coef[:, b : b + 1] * dot(
            rel_emb[...], basis[:, b * width : (b + 1) * width]
        )
    rel_images[...] = folded.astype(BF)

    @tiles(rows, 256)
    def _(block, i):
        own = states[block, :]
        partial[block, :] = dot(own, self_weight[...]) + dot(
            counts[:, block], rel_images[...], 0, 0
        )
        gate[block, :] = lax.logistic(dot(own, gate_weight[...]) + gate_bias[...])


def forward_kernel(
    slots,
    received,
    basis,
    mix,
    degree_inv,
    partial,
    gate,
    states,
    images,
    alpha,
    beta,
):
    rows, width = states.shape
    blocks = basis.shape[1] // width
    part = min(256, slots)
    for b in range(blocks):

        @tiles(slots, part)
        def _(block, i):
            images[pl.ds(pl.multiple_of(b * slots + i * part, part), part), :] = dot(
                received[block, :], basis[:, b * width : (b + 1) * width]
            ).astype(BF)

    @tiles(rows, 256)
    def _(block, i):
        scale = lane_tiled(degree_inv[block, :], width)
        summed = (dot(mix[:, block], images[...], 0, 0) + partial[block, :]) * scale
        aggregated = jnp.tanh(summed)
        opened = gate[block, :]
        alpha[block, :] = opened * (1.0 - aggregated * aggregated) * scale
        beta[block, :] = (
            (aggregated - states[block, :].astype(F32)) * opened * (1.0 - opened)
        )


def upstream_of(block, i, cotangent, handed, handed_slots, export_row):
    total = cotangent[block, :].astype(F32)
    if handed is not None:
        size = total.shape[0]
        slots = export_row.shape[1]
        row = lax.broadcasted_iota(jnp.int32, (size, slots), 0) + i * size
        hot = ones_where(export_row[...] == row)
        total = total + handed[block, :].astype(F32) + dot(hot, handed_slots[...])
    return total


def dense_kernel(first, last, *refs):
    refs = list(refs)
    cotangent, alpha, beta, gate, self_weight, gate_weight = refs[:6]
    refs = refs[6:]
    handed = handed_slots = export_row = None
    if not first:
        handed, handed_slots, export_row = refs[:3]
        refs = refs[3:]
    if last:
        row_grad, dense, gate_row, bias = refs
        bias[...] = jnp.zeros_like(bias)
    else:
        row_grad, dense = refs
    rows = cotangent.shape[0]
    size = 256

    @tiles(rows, size)
    def _(block, i):
        upstream = upstream_of(block, i, cotangent, handed, handed_slots, export_row)
        row_value = (upstream * alpha[block, :]).astype(BF)
        gate_value = upstream * beta[block, :]
        gate_small = gate_value.astype(BF)
        row_grad[block, :] = row_value
        value = (
            upstream * (1.0 - gate[block, :])
            + dot(row_value, self_weight[...], 1, 1)
            + dot(gate_small, gate_weight[...], 1, 1)
        )
        dense[block, :] = value.astype(dense.dtype)
        if last:
            gate_row[block, :] = gate_small
            bias[...] += jnp.sum(gate_value, axis=0, keepdims=True)


def slot_kernel(slots, row_grad, mix, basis, slot_grad, mixed):
    width = row_grad.shape[1]
    blocks = basis.shape[1] // width
    part = min(256, slots)

    @tiles(slots, part)
    def _(block, i):
        total = jnp.zeros((part, width), F32)
        for b in range(blocks):
            at = pl.ds(pl.multiple_of(b * slots + i * part, part), part)
            value = dot(mix[at, :], row_grad[...]).astype(BF)
            mixed[at, :] = value
            total += dot(value, basis[:, b * width : (b + 1) * width], 1, 1)
        slot_grad[block, :] = total.astype(BF)


def weight_kernel(
    slots,
    parts,
    tile_count,
    row_grad,
    gate_row,
    states,
    received,
    mixed,
    counts,
    coef,
    rel_emb,
    basis,
    bias,
    images,
    src_row,
    dst_row,
    rel_row,
    packed,
    scaled,
    edge_grad,
):
    rows, width = states.shape
    relations, blocks = coef.shape
    edges = src_row.shape[1]
    cut = width // parts
    rel_cut = relations // parts
    rel_sum = dot(counts[...], row_grad[...])
    rel_grad = jnp.zeros((relations, width), F32)
    corner = []
    for b in range(blocks):
        columns = slice(b * width, (b + 1) * width)
        value = (coef[:, b : b + 1] * rel_sum).astype(BF)
        scaled[...] = value
        rel_grad += dot(value, basis[:, columns], 1, 1)
        corner.append(
            jnp.sum(
                rel_sum * dot(rel_emb[...], basis[:, columns]), axis=1, keepdims=True
            )
        )
        total = dot(received[...], mixed[b * slots : (b + 1) * slots, :], 0, 0) + dot(
            rel_emb[...], scaled[...], 0, 0
        )
        for p in range(parts):
            packed[p, b * cut : (b + 1) * cut, :] = total[p * cut : (p + 1) * cut].astype(
                BF
            )
    at = blocks * cut
    for grads in (row_grad, gate_row):
        total = dot(states[...], grads[...], 0, 0)
        for p in range(parts):
            packed[p, at : at + cut, :] = total[p * cut : (p + 1) * cut].astype(BF)
        at += cut
    rel_room = rounded_up(rel_cut, 16)
    for p in range(parts):
        value = rel_grad[p * rel_cut : (p + 1) * rel_cut]
        if rel_room > rel_cut:
            value = jnp.concatenate(
                [value, jnp.zeros((rel_room - rel_cut, width), F32)], axis=0
            )
        packed[p, at : at + rel_room, :] = value.astype(BF)
    at += rel_room

    size = 256
    live_edges = tile_count[0, 0] * TILE

    def edge_step(i, sums):
        block = pl.ds(pl.multiple_of(i * size, size), size)
        column = lane_tiled(spread_column(dst_row[:, block]), rows)
        edge = lax.broadcasted_iota(jnp.int32, (size, rows), 0) + i * size
        row = lax.broadcasted_iota(jnp.int32, (size, rows), 1)
        hot = ones_where((column == row) & (edge < live_edges))
        edge_grad[...] = dot(hot, row_grad[...]).astype(BF)
        slot_column = lane_tiled(spread_column(src_row[:, block]), slots)
        own = slot_column == lax.broadcasted_iota(jnp.int32, (size, slots), 1)
        rel_hot = ones_where(
            rel_row[:, block] == lax.broadcasted_iota(jnp.int32, (relations, size), 0)
        )
        out = []
        for b in range(blocks):
            product = dot(edge_grad[...], images[b * slots : (b + 1) * slots, :], 1, 1)
            inner = jnp.sum(
                jnp.where(own, product, jnp.float32(0)), axis=1, keepdims=True
            )
            spread = jnp.broadcast_to(inner, (size, LANES))
            high = spread.astype(BF)
            low = (spread - high.astype(F32)).astype(BF)
            out.append(sums[b] + dot(rel_hot, high) + dot(rel_hot, low))
        return tuple(out)

    sums = lax.fori_loop(
        0,
        edges // size,
        edge_step,
        tuple(jnp.zeros((relations, LANES), F32) for _ in range(blocks)),
    )
    lane = lax.broadcasted_iota(jnp.int32, (relations, LANES), 1)
    gathered = jnp.zeros((relations, LANES), F32)
    for b in range(blocks):
        gathered = jnp.where(lane == b, sums[b] + corner[b], gathered)
    turned = jnp.transpose(gathered)[:8]
    if relations < width:
        turned = jnp.concatenate(
            [turned, jnp.zeros((8, width - relations), F32)], axis=1
        )
    bias8 = jnp.broadcast_to(bias[...], (8, width))
    for p in range(parts):
        rest = packed.shape[1] - at
        lines = [
            turned if p == 0 else pltpu.roll(turned, width - p * rel_cut, 1),
            bias8 if p == 0 else pltpu.roll(bias8, width - p * cut, 1),
        ]
        if rest > 16:
            lines.append(jnp.zeros((rest - 16, width), F32))
        packed[p, at:, :] = jnp.concatenate(lines, axis=0).astype(BF)


def output_kernel(dense, returned, export_row, total):
    rows = dense.shape[0]
    slots = export_row.shape[1]
    size = 256

    @tiles(rows, size)
    def _(block, i):
        row = lax.broadcasted_iota(jnp.int32, (size, slots), 0) + i * size
        hot = ones_where(export_row[...] == row)
        total[block, :] = dense[block, :] + dot(hot, returned[...])


def from_next(block, axis):
    count = lax.axis_size(axis)
    return lax.ppermute(block, axis, [(i, i - 1) for i in range(1, count)])


def halve_over(values, axis):
    count = lax.axis_size(axis)
    index = lax.axis_index(axis)
    distance = 1
    while distance < count:
        left = values.shape[0] // 2
        bit = (index // distance) % 2
        pairs = values.reshape((left, 2) + values.shape[1:])
        sent = lax.dynamic_index_in_dim(pairs, 1 - bit, 1, keepdims=False)
        kept = lax.dynamic_index_in_dim(pairs, bit, 1, keepdims=False)
        route = [(i, i ^ distance) for i in range(count)]
        taken = lax.ppermute(sent, axis, route)
        values = kept.astype(F32) + taken.astype(F32)
        distance *= 2
        if distance < count:
            values = values.astype(BF)
    return values[0]


def per_device(
    states,
    cotangent,
    export_rows,
    edge_src,
    edge_dst,
    edge_rel,
    tile_count,
    basis,
    coef,
    rel_emb,
    self_weight,
    gate_weight,
    gate_bias,
):
    ent_count = lax.axis_size("ent")
    section_count = lax.axis_size("tm")
    own = states[0]
    cot = cotangent[0]
    rows, width = own.shape
    blocks = basis.shape[1] // width
    relations = rel_emb.shape[0]
    edges = edge_src.shape[1]
    slots = export_rows.shape[1]
    per_owner = slots // ent_count

    def exchange(block):
        return lax.all_to_all(
            block.reshape(ent_count, per_owner, width), "ent", 0, 0, tiled=True
        ).reshape(slots, width)

    sent = call(
        export_kernel,
        shape((slots, width), BF),
        (own, export_rows),
        flops=2 * slots * rows * width,
    )
    received = exchange(sent)
    export_next = from_next(export_rows, "tm")
    mix, counts, degree_inv, partial, gate = call(
        functools.partial(setup_kernel, slots),
        (
            shape((blocks * slots, rows), BF),
            shape((relations, rows), BF),
            shape((rows, LANES), F32),
            shape((rows, width), F32),
            shape((rows, width), F32),
        ),
        (
            tile_count,
            edge_src,
            edge_dst,
            edge_rel,
            coef,
            coef.T,
            rel_emb,
            basis,
            own,
            self_weight,
            gate_weight,
            gate_bias[None],
        ),
        scratch=(
            VM((edges, rows), BF),
            VM((blocks, edges), F32),
            VM((relations, width), BF),
        ),
        smem=1,
        flops=2 * blocks * slots * rows * edges,
    )
    images, alpha, beta = call(
        functools.partial(forward_kernel, slots),
        (
            shape((blocks * slots, width), BF),
            shape((rows, width), F32),
            shape((rows, width), F32),
        ),
        (received, basis, mix, degree_inv, partial, gate, own),
        flops=4 * blocks * slots * rows * width,
    )

    handed = None
    for step in range(section_count):
        first, last = step == 0, step + 1 == section_count
        args = (cot, alpha, beta, gate, self_weight, gate_weight)
        if not first:
            args += handed
        outs = (shape((rows, width), BF), shape((rows, width), F32 if last else BF))
        if last:
            outs += (shape((rows, width), BF), shape((1, width), F32))
        outs = call(
            functools.partial(dense_kernel, first, last),
            outs,
            args,
            flops=4 * rows * width * width,
        )
        row_grad, dense = outs[:2]
        slot_grad, mixed = call(
            functools.partial(slot_kernel, slots),
            (shape((slots, width), BF), shape((blocks * slots, width), BF)),
            (row_grad, mix, basis),
            flops=4 * blocks * slots * rows * width,
        )
        if not last:
            ahead = from_next(dense, "tm")
            returned = exchange(slot_grad)
            handed = (ahead, from_next(returned, "tm"), export_next)
    gate_row, bias = outs[2:]

    cut, rel_cut = width // ent_count, relations // ent_count
    rel_room = rounded_up(rel_cut, 16)
    used = (blocks + 2) * cut + rel_room
    depth = rounded_up(used + 16, 16 * section_count)
    packed = call(
        functools.partial(weight_kernel, slots, ent_count),
        shape((ent_count, depth, width), BF),
        (
            tile_count,
            row_grad,
            gate_row,
            own,
            received,
            mixed,
            counts,
            coef,
            rel_emb,
            basis,
            bias,
            images,
            edge_src,
            edge_dst,
            edge_rel,
        ),
        scratch=(VM((relations, width), BF), VM((256, width), BF)),
        smem=1,
        flops=8 * blocks * slots * rows * width,
    )
    returned = exchange(slot_grad)
    state_grad = call(
        output_kernel,
        shape((rows, width), F32),
        (dense, returned, export_rows),
        flops=2 * rows * slots * width,
    )

    own_block = halve_over(packed, "ent").astype(BF)
    quarters = lax.all_to_all(
        own_block.reshape(section_count, depth // section_count, width),
        "tm",
        0,
        0,
        tiled=True,
    )
    quarter = jnp.sum(quarters.astype(F32), axis=0).astype(BF)
    final = lax.all_gather(quarter, "tm", axis=0, tiled=True).astype(F32)
    grad_basis = (
        final[: blocks * cut].reshape(blocks, cut, width).transpose(1, 0, 2)
    ).reshape(cut, blocks * width)
    at = blocks * cut
    grad_self = final[at : at + cut]
    grad_gate = final[at + cut : at + 2 * cut]
    at += 2 * cut
    grad_rel = final[at : at + rel_cut]
    at += rel_room
    grad_coef = final[at : at + blocks, :rel_cut].T
    grad_bias = final[at + 8, :cut]
    return state_grad[None], grad_basis, grad_self, grad_gate, grad_bias, grad_coef, grad_rel


def solution(mesh):
    placed = (P("tm", "ent", None),) * 2 + (P("tm", "ent"),) * 5 + (P(),) * 6
    return jax.shard_map(
        per_device,
        mesh=mesh,
        in_specs=placed,
        out_specs=(
            P("tm", "ent", None),
            P("ent", None),
            P("ent", None),
            P("ent", None),
            P("ent"),
            P("ent", None),
            P("ent", None),
        ),
        check_vma=False,
    )
```

```python
import functools

import jax
import jax.numpy as jnp
from jax import lax
from jax.experimental import pallas as pl
from jax.experimental.pallas import tpu as pltpu
from jax.sharding import PartitionSpec as P

TILE = 128
LANES = 128
BF = jnp.bfloat16
F32 = jnp.float32
VM = pltpu.VMEM


def dot(left, right, left_dim=1, right_dim=0):
    return lax.dot_general(
        left, right, (((left_dim,), (right_dim,)), ((), ())), preferred_element_type=F32
    )


def ones_where(mask):
    return jnp.where(mask, jnp.float32(1), jnp.float32(0)).astype(BF)


def rounded_up(value, unit):
    return -(-value // unit) * unit


def spread_column(row):
    return jnp.transpose(jnp.broadcast_to(row, (LANES, row.shape[1])))


def lane_tiled(column, lanes):
    return jnp.concatenate([column] * (lanes // LANES), axis=1)


ANY = pltpu.HBM
FULL = 63 << 20


def call(kernel, outs, args, scratch=(), flops=0, limit=12 << 20):
    single = not isinstance(outs, list)
    listed = [outs] if single else outs
    out_shape = tuple(shape(dims, kind) for dims, kind, _ in listed)
    out_specs = tuple(pl.BlockSpec(memory_space=place) for _, _, place in listed)
    return pl.pallas_call(
        kernel,
        out_shape=out_shape[0] if single else out_shape,
        in_specs=[pl.BlockSpec(memory_space=place) for _, place in args],
        out_specs=out_specs[0] if single else out_specs,
        scratch_shapes=list(scratch),
        compiler_params=pltpu.CompilerParams(vmem_limit_bytes=limit),
        cost_estimate=pl.CostEstimate(
            flops=flops, bytes_accessed=4 << 20, transcendentals=0
        ),
    )(*[array for array, _ in args])


def fetched(sources, places, sems, start=0):
    copies = []
    for k, (source, place) in enumerate(zip(sources, places)):
        copy = pltpu.make_async_copy(source, place, sems.at[start + k])
        copy.start()
        copies.append(copy)
    return copies


def shape(dims, kind):
    return jax.ShapeDtypeStruct(dims, kind)


def tiles(total, size):
    size = min(total, size)

    def loop(body):
        def step(i, _):
            body(pl.ds(pl.multiple_of(i * size, size), size), i)
            return 0

        lax.fori_loop(0, total // size, step, 0)

    return loop


def export_kernel(states_any, export_any, sent_any, states, export_row, sent, sems):
    rows = states.shape[0]
    slots = export_row.shape[1]
    size = min(256, slots)
    copies = fetched((states_any, export_any), (states, export_row), sems)
    copies[1].wait()
    copies[0].wait()

    @tiles(slots, size)
    def _(block, i):
        column = lane_tiled(spread_column(export_row[:, block]), rows)
        hot = ones_where(column == lax.broadcasted_iota(jnp.int32, (size, rows), 1))
        sent[block, :] = dot(hot, states[...]).astype(BF)

    store = pltpu.make_async_copy(sent, sent_any, sems.at[2])
    store.start()
    store.wait()


def setup_kernel(slots, *refs):
    tile_count = refs[0]
    sources = refs[1:11]
    outs = refs[11:16]
    places = refs[16:26]
    results = refs[26:31]
    target, edge_coef, rel_images, in_sems, out_sems = refs[31:]
    dst_row, rel_row, src_row, coef_t, rel_emb, basis = places[:6]
    states, self_weight, gate_weight, gate_bias = places[6:]
    mix, counts, degree_inv, partial, gate = results
    rows, width = states.shape
    edges = src_row.shape[1]
    blocks, relations = coef_t.shape
    live_edges = tile_count[0, 0] * TILE
    size = 256
    copies = fetched(sources, places, in_sems)
    copies[0].wait()

    @tiles(edges, size)
    def _(block, i):
        column = lane_tiled(spread_column(dst_row[:, block]), rows)
        edge = lax.broadcasted_iota(jnp.int32, (size, rows), 0) + i * size
        row = lax.broadcasted_iota(jnp.int32, (size, rows), 1)
        target[block, :] = ones_where((column == row) & (edge < live_edges))

    copies[1].wait()
    rel_hot = ones_where(
        rel_row[...] == lax.broadcasted_iota(jnp.int32, (relations, edges), 0)
    )
    copies[3].wait()
    edge_coef[...] = dot(coef_t[...].astype(BF), rel_hot)
    counts[...] = dot(rel_hot, target[...]).astype(BF)
    degree = 1.0 + dot(jnp.ones((8, edges), BF), target[...])
    degree_inv[...] = spread_column((1.0 / degree)[:1])
    stores = fetched((counts, degree_inv), outs[1:3], out_sems, 0)
    copies[2].wait()
    part = min(256, slots)
    for b in range(blocks):

        @tiles(slots, part)
        def _(block, i):
            slot = lax.broadcasted_iota(jnp.int32, (part, edges), 0) + i * part
            weighted = jnp.where(
                src_row[...] == slot,
                jnp.broadcast_to(edge_coef[b : b + 1, :], (part, edges)),
                jnp.float32(0),
            ).astype(BF)
            mix[pl.ds(pl.multiple_of(b * slots + i * part, part), part), :] = dot(
                weighted, target[...]
            ).astype(BF)

    stores += fetched((mix,), outs[:1], out_sems, 2)
    copies[4].wait()
    copies[5].wait()
    folded = jnp.zeros((relations, width), F32)
    for b in range(blocks):
        scale = lane_tiled(spread_column(coef_t[b : b + 1, :]), width)
        folded += scale * dot(rel_emb[...], basis[:, b * width : (b + 1) * width])
    rel_images[...] = folded.astype(BF)
    for copy in copies[6:]:
        copy.wait()

    @tiles(rows, 256)
    def _(block, i):
        own = states[block, :]
        partial[block, :] = dot(own, self_weight[...]) + dot(
            counts[:, block], rel_images[...], 0, 0
        )
        gate[block, :] = lax.logistic(dot(own, gate_weight[...]) + gate_bias[...])

    stores += fetched((partial, gate), outs[3:], out_sems, 3)
    for copy in stores:
        copy.wait()


def forward_kernel(slots, *refs):
    received = refs[0]
    sources = refs[1:10]
    basis, mix, gate, self_weight, gate_weight, cotangent = refs[10:16]
    alpha, beta, row_grad, dense, images_any = refs[16:21]
    partial, degree_inv, states, images, sems = refs[21:]
    places = (
        basis,
        mix,
        degree_inv,
        partial,
        gate,
        states,
        cotangent,
        self_weight,
        gate_weight,
    )
    rows, width = states.shape
    blocks = basis.shape[1] // width
    part = min(256, slots)
    copies = fetched(sources, places, sems)
    copies[0].wait()
    for b in range(blocks):

        @tiles(slots, part)
        def _(block, i):
            images[pl.ds(pl.multiple_of(b * slots + i * part, part), part), :] = dot(
                received[block, :], basis[:, b * width : (b + 1) * width]
            ).astype(BF)

    store = pltpu.make_async_copy(images, images_any, sems.at[9])
    store.start()
    for copy in copies[1:]:
        copy.wait()

    @tiles(rows, 256)
    def _(block, i):
        scale = lane_tiled(degree_inv[block, :], width)
        summed = (dot(mix[:, block], images[...], 0, 0) + partial[block, :]) * scale
        aggregated = jnp.tanh(summed)
        opened = gate[block, :]
        row_scale = opened * (1.0 - aggregated * aggregated) * scale
        gate_scale = (
            (aggregated - states[block, :].astype(F32)) * opened * (1.0 - opened)
        )
        alpha[block, :] = row_scale
        beta[block, :] = gate_scale
        upstream = cotangent[block, :].astype(F32)
        row_value = (upstream * row_scale).astype(BF)
        row_grad[block, :] = row_value
        value = (
            upstream * (1.0 - opened)
            + dot(row_value, self_weight[...], 1, 1)
            + dot((upstream * gate_scale).astype(BF), gate_weight[...], 1, 1)
        )
        dense[block, :] = value.astype(dense.dtype)

    store.wait()


def upstream_of(block, i, cotangent, handed, handed_slots, export_row):
    total = cotangent[block, :].astype(F32)
    size = total.shape[0]
    slots = export_row.shape[1]
    row = lax.broadcasted_iota(jnp.int32, (size, slots), 0) + i * size
    hot = ones_where(export_row[...] == row)
    return total + handed[block, :].astype(F32) + dot(hot, handed_slots[...])


def dense_kernel(last, *refs):
    refs = list(refs)
    cotangent, alpha, beta, gate, self_weight, gate_weight = refs[:6]
    refs = refs[6:]
    handed, handed_slots, export_row = refs[:3]
    refs = refs[3:]
    if last:
        row_grad, dense, gate_row, bias = refs
        bias[...] = jnp.zeros_like(bias)
    else:
        row_grad, dense = refs
    rows = cotangent.shape[0]
    size = 256

    @tiles(rows, size)
    def _(block, i):
        upstream = upstream_of(block, i, cotangent, handed, handed_slots, export_row)
        row_value = (upstream * alpha[block, :]).astype(BF)
        gate_value = upstream * beta[block, :]
        gate_small = gate_value.astype(BF)
        row_grad[block, :] = row_value
        value = (
            upstream * (1.0 - gate[block, :])
            + dot(row_value, self_weight[...], 1, 1)
            + dot(gate_small, gate_weight[...], 1, 1)
        )
        dense[block, :] = value.astype(dense.dtype)
        if last:
            gate_row[block, :] = gate_small
            bias[...] += jnp.sum(gate_value, axis=0, keepdims=True)


def slot_kernel(slots, row_grad, mix, basis, slot_grad, mixed):
    width = row_grad.shape[1]
    blocks = basis.shape[1] // width
    part = min(256, slots)

    @tiles(slots, part)
    def _(block, i):
        total = jnp.zeros((part, width), F32)
        for b in range(blocks):
            at = pl.ds(pl.multiple_of(b * slots + i * part, part), part)
            value = dot(mix[at, :], row_grad[...]).astype(BF)
            mixed[at, :] = value
            total += dot(value, basis[:, b * width : (b + 1) * width], 1, 1)
        slot_grad[block, :] = total.astype(BF)


def placer(parts, order):
    me = lax.axis_index("ent")
    even = lax.rem(me, 2) == 0

    def place(i, kept, sent, at, first, second):
        spot = 0
        for k, distance in enumerate(order[1:]):
            mine = lax.rem(lax.div(me, distance), 2)
            bit = 1 - mine if (i // distance) % 2 else mine
            spot = spot + bit * (1 << (len(order) - 2 - k))
        size = first.shape[0]
        kept[spot, at : at + size, :] = jnp.where(even, first, second).astype(BF)
        sent[spot, at : at + size, :] = jnp.where(even, second, first).astype(BF)

    return place


def basis_term(b, slots, received, mixed, coef_t, rel_sum, rel_emb, scaled):
    width = mixed.shape[1]
    scale = lane_tiled(spread_column(coef_t[b : b + 1, :]), width)
    scaled[...] = (scale * rel_sum[...]).astype(BF)
    return dot(received[...], mixed, 0, 0) + dot(rel_emb[...], scaled[...], 0, 0)


def first_weight_kernel(
    slots,
    parts,
    order,
    row_grad,
    gate_row,
    states,
    received,
    mix,
    counts,
    coef_t,
    rel_emb,
    kept,
    sent,
    rel_sum,
    scaled,
    total,
):
    width = states.shape[1]
    cut = width // parts
    place = placer(parts, order)
    rel_sum[...] = dot(counts[...], row_grad[...])

    def put(value, at):
        total[...] = value
        for i in range(0, parts, 2):
            place(
                i,
                kept,
                sent,
                at,
                total[i * cut : (i + 1) * cut, :],
                total[(i + 1) * cut : (i + 2) * cut, :],
            )

    put(dot(states[...], row_grad[...], 0, 0), 0)
    put(dot(states[...], gate_row[...], 0, 0), cut)
    mixed = dot(mix[:slots, :], row_grad[...]).astype(BF)
    put(basis_term(0, slots, received, mixed, coef_t, rel_sum, rel_emb, scaled), 2 * cut)


def second_weight_kernel(
    slots,
    parts,
    order,
    tile_count,
    row_grad,
    received,
    mixed,
    coef_t,
    rel_emb,
    basis,
    bias,
    images,
    rel_sum,
    src_row,
    dst_row,
    rel_row,
    kept,
    sent,
    scaled,
    total,
    edge_grad,
):
    rows, width = row_grad.shape
    blocks, relations = coef_t.shape
    edges = src_row.shape[1]
    cut = width // parts
    rel_cut = relations // parts
    rel_room = rounded_up(rel_cut, 16)
    place = placer(parts, order)
    rel_grad = jnp.zeros((relations, width), F32)
    corner = []
    for b in range(blocks):
        columns = slice(b * width, (b + 1) * width)
        corner.append(
            jnp.sum(
                rel_sum[...] * dot(rel_emb[...], basis[:, columns]),
                axis=1,
                keepdims=True,
            )
        )
        term = basis_term(
            b,
            slots,
            received,
            mixed[b * slots : (b + 1) * slots, :],
            coef_t,
            rel_sum,
            rel_emb,
            scaled,
        ) if b else None
        if not b:
            scale = lane_tiled(spread_column(coef_t[:1, :]), width)
            scaled[...] = (scale * rel_sum[...]).astype(BF)
        rel_grad += dot(scaled[...], basis[:, columns], 1, 1)
        if b:
            total[...] = term
            for i in range(0, parts, 2):
                place(
                    i,
                    kept,
                    sent,
                    (b - 1) * cut,
                    total[i * cut : (i + 1) * cut, :],
                    total[(i + 1) * cut : (i + 2) * cut, :],
                )

    size = 256
    live_edges = tile_count[0, 0] * TILE

    def edge_step(i, sums):
        block = pl.ds(pl.multiple_of(i * size, size), size)
        column = lane_tiled(spread_column(dst_row[:, block]), rows)
        edge = lax.broadcasted_iota(jnp.int32, (size, rows), 0) + i * size
        row = lax.broadcasted_iota(jnp.int32, (size, rows), 1)
        hot = ones_where((column == row) & (edge < live_edges))
        edge_grad[...] = dot(hot, row_grad[...]).astype(BF)
        slot_column = lane_tiled(spread_column(src_row[:, block]), slots)
        own = slot_column == lax.broadcasted_iota(jnp.int32, (size, slots), 1)
        rel_hot = ones_where(
            rel_row[:, block] == lax.broadcasted_iota(jnp.int32, (relations, size), 0)
        )
        lane = lax.broadcasted_iota(jnp.int32, (size, LANES), 1)
        inner = jnp.zeros((size, LANES), F32)
        for b in range(blocks):
            product = dot(edge_grad[...], images[b * slots : (b + 1) * slots, :], 1, 1)
            value = jnp.sum(
                jnp.where(own, product, jnp.float32(0)), axis=1, keepdims=True
            )
            inner = jnp.where(lane == b, value, inner)
        high = inner.astype(BF)
        low = (inner - high.astype(F32)).astype(BF)
        return sums + dot(rel_hot, high) + dot(rel_hot, low)

    gathered = lax.fori_loop(
        0, edges // size, edge_step, jnp.zeros((relations, LANES), F32)
    )
    lane = lax.broadcasted_iota(jnp.int32, (relations, LANES), 1)
    for b in range(blocks):
        gathered = gathered + jnp.where(lane == b, corner[b], jnp.float32(0))
    turned = jnp.transpose(gathered)[:8]
    if relations < width:
        turned = jnp.concatenate(
            [turned, jnp.zeros((8, width - relations), F32)], axis=1
        )
    bias8 = jnp.broadcast_to(bias[...], (8, width))
    at = (blocks - 1) * cut
    rest = kept.shape[1] - at - rel_room

    def last_rows(p):
        lines = [rel_grad[p * rel_cut : (p + 1) * rel_cut]]
        if rel_room > rel_cut:
            lines.append(jnp.zeros((rel_room - rel_cut, width), F32))
        lines.append(turned if p == 0 else pltpu.roll(turned, width - p * rel_cut, 1))
        lines.append(bias8 if p == 0 else pltpu.roll(bias8, width - p * cut, 1))
        if rest > 16:
            lines.append(jnp.zeros((rest - 16, width), F32))
        return jnp.concatenate(lines, axis=0)

    for i in range(0, parts, 2):
        place(i, kept, sent, at, last_rows(i), last_rows(i + 1))


def fold_kernel(kept, taken, next_kept, next_sent):
    left = next_kept.shape[0]
    for spot in range(left):
        next_kept[spot] = (kept[spot].astype(F32) + taken[spot].astype(F32)).astype(BF)
        other = left + spot
        next_sent[spot] = (kept[other].astype(F32) + taken[other].astype(F32)).astype(BF)


def join_kernel(kept_a, taken_a, kept_b, taken_b, joined):
    parts = [
        kept_a[0].astype(F32) + taken_a[0].astype(F32),
        kept_b[0].astype(F32) + taken_b[0].astype(F32),
    ]
    whole = jnp.concatenate(parts, axis=0).astype(BF)
    size = joined.shape[1]
    for k in range(joined.shape[0]):
        joined[k] = whole[k * size : (k + 1) * size]


def quarter_kernel(taken, total):
    value = taken[0].astype(F32)
    for k in range(1, taken.shape[0]):
        value += taken[k].astype(F32)
    total[...] = value.astype(BF)


def final_kernel(final, basis, self_part, gate_part, rel, coef_t, bias):
    cut, width = self_part.shape
    blocks, rel_cut = coef_t.shape
    value = final[...].astype(F32)
    self_part[...] = value[:cut]
    gate_part[...] = value[cut : 2 * cut]
    for b in range(blocks):
        basis[:, b * width : (b + 1) * width] = value[(b + 2) * cut : (b + 3) * cut]
    at = (blocks + 2) * cut
    rel[...] = value[at : at + rel_cut]
    at += rounded_up(rel_cut, 16)
    coef_t[...] = value[at : at + blocks, :rel_cut]
    bias[...] = value[at + 8 : at + 9, :cut]


def output_kernel(dense, returned, export_row, total):
    rows = dense.shape[0]
    slots = export_row.shape[1]
    size = 256

    @tiles(rows, size)
    def _(block, i):
        row = lax.broadcasted_iota(jnp.int32, (size, slots), 0) + i * size
        hot = ones_where(export_row[...] == row)
        total[block, :] = dense[block, :] + dot(hot, returned[...])


def from_next(block, axis):
    count = lax.axis_size(axis)
    return lax.ppermute(block, axis, [(i, i - 1) for i in range(1, count)])


def per_device(
    states,
    cotangent,
    export_rows,
    edge_src,
    edge_dst,
    edge_rel,
    tile_count,
    basis,
    coef,
    rel_emb,
    self_weight,
    gate_weight,
    gate_bias,
):
    ent_count = lax.axis_size("ent")
    section_count = lax.axis_size("tm")
    own = states[0]
    cot = cotangent[0]
    rows, width = own.shape
    blocks = basis.shape[1] // width
    relations = rel_emb.shape[0]
    edges = edge_src.shape[1]
    slots = export_rows.shape[1]
    per_owner = slots // ent_count

    def exchange(block):
        return lax.all_to_all(
            block.reshape(ent_count, per_owner, width), "ent", 0, 0, tiled=True
        ).reshape(slots, width)

    dma = pltpu.SemaphoreType.DMA
    sent = call(
        export_kernel,
        ((slots, width), BF, ANY),
        [(own, ANY), (export_rows, ANY)],
        scratch=(
            VM((rows, width), BF),
            VM((1, slots), jnp.int32),
            VM((slots, width), BF),
            dma((3,)),
        ),
        flops=2 * slots * rows * width,
        limit=FULL,
    )
    received = exchange(sent)
    export_next = from_next(export_rows, "tm")
    coef_t = coef.T
    bias_row = gate_bias[None]
    sources = [
        edge_dst,
        edge_rel,
        edge_src,
        coef_t,
        rel_emb,
        basis,
        own,
        self_weight,
        gate_weight,
        bias_row,
    ]
    made = [
        ((blocks * slots, rows), BF),
        ((relations, rows), BF),
        ((rows, LANES), F32),
        ((rows, width), F32),
        ((rows, width), F32),
    ]
    mix, counts, degree_inv, partial, gate = call(
        functools.partial(setup_kernel, slots),
        [out + (ANY,) for out in made],
        [(tile_count, pltpu.SMEM)] + [(array, ANY) for array in sources],
        scratch=[VM(array.shape, array.dtype) for array in sources]
        + [VM(dims, kind) for dims, kind in made]
        + [
            VM((edges, rows), BF),
            VM((blocks, edges), F32),
            VM((relations, width), BF),
            dma((len(sources),)),
            dma((len(made),)),
        ],
        flops=2 * blocks * slots * rows * edges,
        limit=FULL,
    )
    outs = call(
        functools.partial(forward_kernel, slots),
        [
            (basis.shape, BF, VM),
            (mix.shape, BF, VM),
            ((rows, width), F32, VM),
            ((width, width), BF, VM),
            ((width, width), BF, VM),
            ((rows, width), BF, VM),
            ((rows, width), F32, VM),
            ((rows, width), F32, VM),
            ((rows, width), BF, VM),
            ((rows, width), BF, VM),
            ((blocks * slots, width), BF, ANY),
        ],
        [(received, VM)]
        + [
            (array, ANY)
            for array in (
                basis,
                mix,
                degree_inv,
                partial,
                gate,
                own,
                cot,
                self_weight,
                gate_weight,
            )
        ],
        scratch=[
            VM((rows, width), F32),
            VM((rows, LANES), F32),
            VM((rows, width), BF),
            VM((blocks * slots, width), BF),
            dma((10,)),
        ],
        flops=4 * blocks * slots * rows * width,
        limit=FULL - (16 << 20),
    )
    basis_near, mix_near, gate_near, self_near, gate_weight_near, cot_near = outs[:6]
    alpha, beta, row_grad, dense, images = outs[6:]

    def slot_step(row_grad):
        return call(
            functools.partial(slot_kernel, slots),
            [((slots, width), BF, VM), ((blocks * slots, width), BF, VM)],
            [(row_grad, VM), (mix_near, VM), (basis_near, VM)],
            flops=4 * blocks * slots * rows * width,
        )

    for step in range(1, section_count):
        last = step + 1 == section_count
        slot_grad, _ = slot_step(row_grad)
        ahead = from_next(dense, "tm")
        returned = from_next(exchange(slot_grad), "tm")
        args = [cot_near, alpha, beta, gate_near, self_near, gate_weight_near]
        args += [ahead, returned, export_next]
        outs = [((rows, width), BF, VM), ((rows, width), F32 if last else BF, VM)]
        if last:
            outs += [((rows, width), BF, VM), ((1, width), F32, VM)]
        outs = call(
            functools.partial(dense_kernel, last),
            outs,
            [(array, VM) for array in args],
            flops=4 * rows * width * width,
        )
        row_grad, dense = outs[:2]
    gate_row, bias = outs[2:]

    cut, rel_cut = width // ent_count, relations // ent_count
    first_depth = 3 * cut
    rest = (blocks - 1) * cut + rounded_up(rel_cut, 16) + 16
    depth = rounded_up(first_depth + rest, 16 * section_count)
    distances = []
    while 1 << len(distances) < ent_count:
        distances.append(1 << len(distances))
    orders = (distances, distances[:1] + distances[:0:-1])
    half = ent_count // 2
    kept_a, sent_a, rel_sum = call(
        functools.partial(first_weight_kernel, slots, ent_count, orders[0]),
        [
            ((half, first_depth, width), BF, VM),
            ((half, first_depth, width), BF, VM),
            ((relations, width), F32, VM),
        ],
        [
            (array, VM)
            for array in (
                row_grad,
                gate_row,
                own,
                received,
                mix_near,
                counts,
                coef_t,
                rel_emb,
            )
        ],
        scratch=[VM((relations, width), BF), VM((width, width), F32)],
        flops=4 * rows * width * width,
    )
    slot_grad, mixed = slot_step(row_grad)
    kept_b, sent_b = call(
        functools.partial(second_weight_kernel, slots, ent_count, orders[1]),
        [((half, depth - first_depth, width), BF, VM)] * 2,
        [(tile_count, pltpu.SMEM)]
        + [
            (array, VM)
            for array in (
                row_grad,
                received,
                mixed,
                coef_t,
                rel_emb,
                basis_near,
                bias,
                images,
                rel_sum,
                edge_src,
                edge_dst,
                edge_rel,
            )
        ],
        scratch=[
            VM((relations, width), BF),
            VM((width, width), F32),
            VM((256, width), BF),
        ],
        flops=8 * blocks * slots * rows * width,
    )
    folds = [(kept_a, sent_a), (kept_b, sent_b)]
    taken = [None, None]
    for k in range(len(distances)):
        for which in range(2):
            kept, moved = folds[which]
            distance = orders[which][k]
            route = [(i, i ^ distance) for i in range(ent_count)]
            taken[which] = lax.ppermute(moved, "ent", route)
        if k + 1 < len(distances):
            for which in range(2):
                kept = folds[which][0]
                dims = (kept.shape[0] // 2,) + kept.shape[1:]
                folds[which] = call(
                    fold_kernel,
                    [(dims, BF, VM)] * 2,
                    [(kept, VM), (taken[which], VM)],
                    flops=1 << 20,
                )
    joined = call(
        join_kernel,
        ((section_count, depth // section_count, width), BF, VM),
        [(folds[0][0], VM), (taken[0], VM), (folds[1][0], VM), (taken[1], VM)],
        flops=1 << 20,
    )
    returned = exchange(slot_grad)
    state_grad = call(
        output_kernel,
        ((rows, width), F32, VM),
        [(dense, VM), (returned, VM), (export_rows, VM)],
        flops=2 * rows * slots * width,
    )
    quarter = call(
        quarter_kernel,
        ((depth // section_count, width), BF, VM),
        [(lax.all_to_all(joined, "tm", 0, 0, tiled=True), VM)],
        flops=1 << 20,
    )
    final = lax.all_gather(quarter, "tm", axis=0, tiled=True)
    grad_basis, grad_self, grad_gate, grad_rel, grad_coef, grad_bias = call(
        final_kernel,
        [
            ((cut, blocks * width), F32, VM),
            ((cut, width), F32, VM),
            ((cut, width), F32, VM),
            ((rel_cut, width), F32, VM),
            ((blocks, rel_cut), F32, VM),
            ((1, cut), F32, VM),
        ],
        [(final, VM)],
        flops=1 << 20,
    )
    return (
        state_grad[None],
        grad_basis,
        grad_self,
        grad_gate,
        grad_bias[0],
        grad_coef.T,
        grad_rel,
    )


def solution(mesh):
    placed = (P("tm", "ent", None),) * 2 + (P("tm", "ent"),) * 5 + (P(),) * 6
    return jax.shard_map(
        per_device,
        mesh=mesh,
        in_specs=placed,
        out_specs=(
            P("tm", "ent", None),
            P("ent", None),
            P("ent", None),
            P("ent", None),
            P("ent"),
            P("ent", None),
            P("ent", None),
        ),
        check_vma=False,
    )
```

```python
import functools

import jax
import jax.numpy as jnp
from jax import lax
from jax.experimental import pallas as pl
from jax.experimental.pallas import tpu as pltpu
from jax.sharding import PartitionSpec as P

TILE = 128
LANES = 128
BF = jnp.bfloat16
F32 = jnp.float32
VM = pltpu.VMEM


def dot(left, right, left_dim=1, right_dim=0):
    return lax.dot_general(
        left, right, (((left_dim,), (right_dim,)), ((), ())), preferred_element_type=F32
    )


def ones_where(mask):
    return jnp.where(mask, jnp.float32(1), jnp.float32(0)).astype(BF)


def rounded_up(value, unit):
    return -(-value // unit) * unit


def spread_column(row):
    return jnp.transpose(jnp.broadcast_to(row, (LANES, row.shape[1])))


def lane_tiled(column, lanes):
    return jnp.concatenate([column] * (lanes // LANES), axis=1)


ANY = pltpu.HBM
FULL = 63 << 20
LIGHT = 1 << 20


def call(kernel, outs, args, scratch=(), flops=0, limit=12 << 20):
    single = not isinstance(outs, list)
    listed = [outs] if single else outs
    out_shape = tuple(shape(dims, kind) for dims, kind, _ in listed)
    out_specs = tuple(pl.BlockSpec(memory_space=place) for _, _, place in listed)
    return pl.pallas_call(
        kernel,
        out_shape=out_shape[0] if single else out_shape,
        in_specs=[pl.BlockSpec(memory_space=place) for _, place in args],
        out_specs=out_specs[0] if single else out_specs,
        scratch_shapes=list(scratch),
        compiler_params=pltpu.CompilerParams(vmem_limit_bytes=limit),
        cost_estimate=pl.CostEstimate(
            flops=flops, bytes_accessed=4 << 20, transcendentals=0
        ),
    )(*[array for array, _ in args])


def fetched(sources, places, sems, start=0):
    copies = []
    for k, (source, place) in enumerate(zip(sources, places)):
        copy = pltpu.make_async_copy(source, place, sems.at[start + k])
        copy.start()
        copies.append(copy)
    return copies


def shape(dims, kind):
    return jax.ShapeDtypeStruct(dims, kind)


def tiles(total, size):
    size = min(total, size)

    def loop(body):
        def step(i, _):
            body(pl.ds(pl.multiple_of(i * size, size), size), i)
            return 0

        lax.fori_loop(0, total // size, step, 0)

    return loop


def export_kernel(states_any, export_any, sent_any, states, export_row, sent, sems):
    rows = states.shape[0]
    slots = export_row.shape[1]
    size = min(256, slots)
    copies = fetched((states_any, export_any), (states, export_row), sems)
    copies[1].wait()
    copies[0].wait()

    @tiles(slots, size)
    def _(block, i):
        column = lane_tiled(spread_column(export_row[:, block]), rows)
        hot = ones_where(column == lax.broadcasted_iota(jnp.int32, (size, rows), 1))
        sent[block, :] = dot(hot, states[...]).astype(BF)

    store = pltpu.make_async_copy(sent, sent_any, sems.at[2])
    store.start()
    store.wait()


def setup_kernel(slots, *refs):
    tile_count = refs[0]
    sources, outs = refs[1:7], refs[7:11]
    places, results = refs[11:17], refs[17:21]
    target, edge_coef, in_sems, out_sems = refs[21:]
    dst_row, rel_row, src_row, coef_t, rel_emb, basis = places
    mix, counts, degree_inv, rel_images = results
    edges, rows = target.shape
    width = rel_emb.shape[1]
    blocks, relations = coef_t.shape
    live_edges = tile_count[0, 0] * TILE
    size = 256
    copies = fetched(sources, places, in_sems)
    copies[0].wait()

    @tiles(edges, size)
    def _(block, i):
        column = lane_tiled(spread_column(dst_row[:, block]), rows)
        edge = lax.broadcasted_iota(jnp.int32, (size, rows), 0) + i * size
        row = lax.broadcasted_iota(jnp.int32, (size, rows), 1)
        target[block, :] = ones_where((column == row) & (edge < live_edges))

    copies[1].wait()
    rel_hot = ones_where(
        rel_row[...] == lax.broadcasted_iota(jnp.int32, (relations, edges), 0)
    )
    copies[3].wait()
    edge_coef[...] = dot(coef_t[...].astype(BF), rel_hot)
    copies[2].wait()
    part = min(256, slots)
    stores = []
    for b in range(blocks):

        @tiles(slots, part)
        def _(block, i):
            slot = lax.broadcasted_iota(jnp.int32, (part, edges), 0) + i * part
            weighted = jnp.where(
                src_row[...] == slot,
                jnp.broadcast_to(edge_coef[b : b + 1, :], (part, edges)),
                jnp.float32(0),
            ).astype(BF)
            mix[pl.ds(pl.multiple_of(b * slots + i * part, part), part), :] = dot(
                weighted, target[...]
            ).astype(BF)

        lines = pl.ds(b * slots, slots)
        stores += fetched((mix.at[lines],), (outs[0].at[lines],), out_sems, b)
    counts[...] = dot(rel_hot, target[...]).astype(BF)
    degree = 1.0 + dot(jnp.ones((8, edges), BF), target[...])
    degree_inv[...] = spread_column((1.0 / degree)[:1])
    stores += fetched((counts, degree_inv), outs[1:3], out_sems, blocks)
    copies[4].wait()
    copies[5].wait()
    folded = jnp.zeros((relations, width), F32)
    for b in range(blocks):
        scale = lane_tiled(spread_column(coef_t[b : b + 1, :]), width)
        folded += scale * dot(rel_emb[...], basis[:, b * width : (b + 1) * width])
    rel_images[...] = folded.astype(BF)
    stores += fetched((rel_images,), outs[3:], out_sems, blocks + 2)
    for copy in stores:
        copy.wait()


def forward_kernel(slots, *refs):
    sources, outs = refs[:11], refs[11:17]
    places, results = refs[17:28], refs[28:34]
    in_sems, tile_sems, store_sem = refs[34:]
    received, basis, mix, self_weight, gate_weight, gate_bias = places[:6]
    counts, rel_images, degree_inv, states, cotangent = places[6:]
    dense, row_grad, gate, alpha, beta, images = results
    rows, width = states.shape
    blocks = basis.shape[1] // width
    part = min(256, slots)
    copies = fetched(sources, places, in_sems)
    copies[0].wait()
    copies[1].wait()
    for b in range(blocks):

        @tiles(slots, part)
        def _(block, i):
            images[pl.ds(pl.multiple_of(b * slots + i * part, part), part), :] = dot(
                received[block, :], basis[:, b * width : (b + 1) * width]
            ).astype(BF)

    store = pltpu.make_async_copy(images, outs[5], store_sem)
    store.start()
    for copy in copies[2:]:
        copy.wait()

    def tile_copies(block, i):
        return [
            pltpu.make_async_copy(results[k].at[block], outs[k].at[block], tile_sems.at[k, i])
            for k in range(5)
        ]

    @tiles(rows, 256)
    def _(block, i):
        own = states[block, :]
        scale = lane_tiled(degree_inv[block, :], width)
        summed = (
            dot(mix[:, block], images[...], 0, 0)
            + dot(counts[:, block], rel_images[...], 0, 0)
            + dot(own, self_weight[...])
        ) * scale
        aggregated = jnp.tanh(summed)
        opened = lax.logistic(dot(own, gate_weight[...]) + gate_bias[...])
        row_scale = opened * (1.0 - aggregated * aggregated) * scale
        gate_scale = (aggregated - own.astype(F32)) * opened * (1.0 - opened)
        gate[block, :] = opened
        alpha[block, :] = row_scale
        beta[block, :] = gate_scale
        upstream = cotangent[block, :].astype(F32)
        row_value = (upstream * row_scale).astype(BF)
        row_grad[block, :] = row_value
        value = (
            upstream * (1.0 - opened)
            + dot(row_value, self_weight[...], 1, 1)
            + dot((upstream * gate_scale).astype(BF), gate_weight[...], 1, 1)
        )
        dense[block, :] = value.astype(dense.dtype)
        for copy in tile_copies(block, i):
            copy.start()

    @tiles(rows, 256)
    def _(block, i):
        for copy in tile_copies(block, i):
            copy.wait()

    store.wait()


def upstream_of(block, i, cotangent, handed, handed_slots, export_row):
    total = cotangent[block, :].astype(F32)
    size = total.shape[0]
    slots = export_row.shape[1]
    row = lax.broadcasted_iota(jnp.int32, (size, slots), 0) + i * size
    hot = ones_where(export_row[...] == row)
    return total + handed[block, :].astype(F32) + dot(hot, handed_slots[...])


def dense_kernel(last, *refs):
    refs = list(refs)
    cotangent, alpha, beta, gate, self_weight, gate_weight = refs[:6]
    refs = refs[6:]
    handed, handed_slots, export_row = refs[:3]
    refs = refs[3:]
    if last:
        row_grad, dense, gate_row, bias = refs
        bias[...] = jnp.zeros_like(bias)
    else:
        row_grad, dense = refs
    rows = cotangent.shape[0]
    size = 256

    @tiles(rows, size)
    def _(block, i):
        upstream = upstream_of(block, i, cotangent, handed, handed_slots, export_row)
        row_value = (upstream * alpha[block, :]).astype(BF)
        gate_value = upstream * beta[block, :]
        gate_small = gate_value.astype(BF)
        row_grad[block, :] = row_value
        value = (
            upstream * (1.0 - gate[block, :])
            + dot(row_value, self_weight[...], 1, 1)
            + dot(gate_small, gate_weight[...], 1, 1)
        )
        dense[block, :] = value.astype(dense.dtype)
        if last:
            gate_row[block, :] = gate_small
            bias[...] += jnp.sum(gate_value, axis=0, keepdims=True)


def slot_kernel(slots, row_grad, mix, basis, slot_grad, mixed):
    width = row_grad.shape[1]
    blocks = basis.shape[1] // width
    part = min(256, slots)

    @tiles(slots, part)
    def _(block, i):
        total = jnp.zeros((part, width), F32)
        for b in range(blocks):
            at = pl.ds(pl.multiple_of(b * slots + i * part, part), part)
            value = dot(mix[at, :], row_grad[...]).astype(BF)
            mixed[at, :] = value
            total += dot(value, basis[:, b * width : (b + 1) * width], 1, 1)
        slot_grad[block, :] = total.astype(BF)


def placer(parts, order):
    me = lax.axis_index("ent")
    even = lax.rem(me, 2) == 0

    def place(i, kept, sent, at, first, second):
        spot = 0
        for k, distance in enumerate(order[1:]):
            mine = lax.rem(lax.div(me, distance), 2)
            bit = 1 - mine if (i // distance) % 2 else mine
            spot = spot + bit * (1 << (len(order) - 2 - k))
        size = first.shape[0]
        kept[spot, at : at + size, :] = jnp.where(even, first, second).astype(BF)
        sent[spot, at : at + size, :] = jnp.where(even, second, first).astype(BF)

    return place


def basis_term(b, slots, received, mixed, coef_t, rel_sum, rel_emb, scaled):
    width = mixed.shape[1]
    scale = lane_tiled(spread_column(coef_t[b : b + 1, :]), width)
    scaled[...] = (scale * rel_sum[...]).astype(BF)
    return dot(received[...], mixed, 0, 0) + dot(rel_emb[...], scaled[...], 0, 0)


def first_weight_kernel(
    slots,
    parts,
    order,
    row_grad,
    gate_row,
    states,
    received,
    mix,
    counts,
    coef_t,
    rel_emb,
    kept,
    sent,
    rel_sum,
    scaled,
    total,
):
    width = states.shape[1]
    cut = width // parts
    place = placer(parts, order)
    rel_sum[...] = dot(counts[...], row_grad[...])

    def put(value, at):
        total[...] = value
        for i in range(0, parts, 2):
            place(
                i,
                kept,
                sent,
                at,
                total[i * cut : (i + 1) * cut, :],
                total[(i + 1) * cut : (i + 2) * cut, :],
            )

    put(dot(states[...], row_grad[...], 0, 0), 0)
    put(dot(states[...], gate_row[...], 0, 0), cut)
    mixed = dot(mix[:slots, :], row_grad[...]).astype(BF)
    put(basis_term(0, slots, received, mixed, coef_t, rel_sum, rel_emb, scaled), 2 * cut)


def second_weight_kernel(
    slots,
    parts,
    order,
    received,
    mixed,
    coef_t,
    rel_emb,
    rel_sum,
    kept,
    sent,
    scaled,
    total,
):
    width = received.shape[1]
    cut = width // parts
    place = placer(parts, order)
    for b in range(1, coef_t.shape[0]):
        lines = mixed[b * slots : (b + 1) * slots, :]
        total[...] = basis_term(
            b, slots, received, lines, coef_t, rel_sum, rel_emb, scaled
        )
        for i in range(0, parts, 2):
            place(
                i,
                kept,
                sent,
                (b - 1) * cut,
                total[i * cut : (i + 1) * cut, :],
                total[(i + 1) * cut : (i + 2) * cut, :],
            )


def third_weight_kernel(
    slots,
    parts,
    tile_count,
    row_grad,
    slot_grad,
    coef_t,
    rel_emb,
    basis,
    bias,
    images,
    rel_sum,
    src_row,
    dst_row,
    rel_row,
    packed,
    scaled,
    edge_grad,
):
    rows, width = row_grad.shape
    blocks, relations = coef_t.shape
    edges = src_row.shape[1]
    cut = width // parts
    rel_cut = relations // parts
    rel_room = rounded_up(rel_cut, 16)
    per_owner = slots // parts
    for p in range(parts):
        packed[p, :per_owner, :] = slot_grad[p * per_owner : (p + 1) * per_owner, :]
    rel_grad = jnp.zeros((relations, width), F32)
    corner = []
    for b in range(blocks):
        columns = slice(b * width, (b + 1) * width)
        corner.append(
            jnp.sum(
                rel_sum[...] * dot(rel_emb[...], basis[:, columns]),
                axis=1,
                keepdims=True,
            )
        )
        scale = lane_tiled(spread_column(coef_t[b : b + 1, :]), width)
        scaled[...] = (scale * rel_sum[...]).astype(BF)
        rel_grad += dot(scaled[...], basis[:, columns], 1, 1)

    size = 256
    live_edges = tile_count[0, 0] * TILE

    def edge_step(i, sums):
        block = pl.ds(pl.multiple_of(i * size, size), size)
        column = lane_tiled(spread_column(dst_row[:, block]), rows)
        edge = lax.broadcasted_iota(jnp.int32, (size, rows), 0) + i * size
        row = lax.broadcasted_iota(jnp.int32, (size, rows), 1)
        hot = ones_where((column == row) & (edge < live_edges))
        edge_grad[...] = dot(hot, row_grad[...]).astype(BF)
        slot_column = lane_tiled(spread_column(src_row[:, block]), slots)
        own = slot_column == lax.broadcasted_iota(jnp.int32, (size, slots), 1)
        rel_hot = ones_where(
            rel_row[:, block] == lax.broadcasted_iota(jnp.int32, (relations, size), 0)
        )
        lane = lax.broadcasted_iota(jnp.int32, (size, LANES), 1)
        inner = jnp.zeros((size, LANES), F32)
        for b in range(blocks):
            product = dot(edge_grad[...], images[b * slots : (b + 1) * slots, :], 1, 1)
            value = jnp.sum(
                jnp.where(own, product, jnp.float32(0)), axis=1, keepdims=True
            )
            inner = jnp.where(lane == b, value, inner)
        high = inner.astype(BF)
        low = (inner - high.astype(F32)).astype(BF)
        return sums + dot(rel_hot, high) + dot(rel_hot, low)

    gathered = lax.fori_loop(
        0, edges // size, edge_step, jnp.zeros((relations, LANES), F32)
    )
    lane = lax.broadcasted_iota(jnp.int32, (relations, LANES), 1)
    for b in range(blocks):
        gathered = gathered + jnp.where(lane == b, corner[b], jnp.float32(0))
    turned = jnp.transpose(gathered)[:8]
    if relations < width:
        turned = jnp.concatenate(
            [turned, jnp.zeros((8, width - relations), F32)], axis=1
        )
    bias8 = jnp.broadcast_to(bias[...], (8, width))
    for p in range(parts):
        lines = [rel_grad[p * rel_cut : (p + 1) * rel_cut]]
        if rel_room > rel_cut:
            lines.append(jnp.zeros((rel_room - rel_cut, width), F32))
        lines.append(turned if p == 0 else pltpu.roll(turned, width - p * rel_cut, 1))
        lines.append(bias8 if p == 0 else pltpu.roll(bias8, width - p * cut, 1))
        packed[p, per_owner:, :] = jnp.concatenate(lines, axis=0).astype(BF)


def fold_kernel(kept, taken, next_kept, next_sent):
    left = next_kept.shape[0]
    for spot in range(left):
        next_kept[spot] = (kept[spot].astype(F32) + taken[spot].astype(F32)).astype(BF)
        other = left + spot
        next_sent[spot] = (kept[other].astype(F32) + taken[other].astype(F32)).astype(BF)


def join_kernel(per_owner, kept_a, taken_a, kept_b, taken_b, packed, joined):
    size, width = joined.shape[1:]
    rest = packed[0, per_owner:, :].astype(F32)
    for k in range(1, packed.shape[0]):
        rest += packed[k, per_owner:, :].astype(F32)
    parts = [
        kept_a[0].astype(F32) + taken_a[0].astype(F32),
        kept_b[0].astype(F32) + taken_b[0].astype(F32),
        rest,
    ]
    unused = size * joined.shape[0] - sum(part.shape[0] for part in parts)
    if unused:
        parts.append(jnp.zeros((unused, width), F32))
    whole = jnp.concatenate(parts, axis=0).astype(BF)
    for k in range(joined.shape[0]):
        joined[k] = whole[k * size : (k + 1) * size]


def quarter_kernel(taken, total):
    value = taken[0].astype(F32)
    for k in range(1, taken.shape[0]):
        value += taken[k].astype(F32)
    total[...] = value.astype(BF)


def final_kernel(final, basis, self_part, gate_part, rel, coef_t, bias):
    cut, width = self_part.shape
    blocks, rel_cut = coef_t.shape
    value = final[...].astype(F32)
    self_part[...] = value[:cut]
    gate_part[...] = value[cut : 2 * cut]
    for b in range(blocks):
        basis[:, b * width : (b + 1) * width] = value[(b + 2) * cut : (b + 3) * cut]
    at = (blocks + 2) * cut
    rel[...] = value[at : at + rel_cut]
    at += rounded_up(rel_cut, 16)
    coef_t[...] = value[at : at + blocks, :rel_cut]
    bias[...] = value[at + 8 : at + 9, :cut]


def output_kernel(dense, packed, export_row, total, returned):
    rows = dense.shape[0]
    slots = export_row.shape[1]
    parts = packed.shape[0]
    per_owner = slots // parts
    size = 256
    for p in range(parts):
        returned[p * per_owner : (p + 1) * per_owner, :] = packed[p, :per_owner, :]

    @tiles(rows, size)
    def _(block, i):
        row = lax.broadcasted_iota(jnp.int32, (size, slots), 0) + i * size
        hot = ones_where(export_row[...] == row)
        total[block, :] = dense[block, :] + dot(hot, returned[...])


def from_next(block, axis):
    count = lax.axis_size(axis)
    return lax.ppermute(block, axis, [(i, i - 1) for i in range(1, count)])


def per_device(
    states,
    cotangent,
    export_rows,
    edge_src,
    edge_dst,
    edge_rel,
    tile_count,
    basis,
    coef,
    rel_emb,
    self_weight,
    gate_weight,
    gate_bias,
):
    ent_count = lax.axis_size("ent")
    section_count = lax.axis_size("tm")
    own = states[0]
    cot = cotangent[0]
    rows, width = own.shape
    blocks = basis.shape[1] // width
    relations = rel_emb.shape[0]
    edges = edge_src.shape[1]
    slots = export_rows.shape[1]
    per_owner = slots // ent_count

    def exchange(block):
        return lax.all_to_all(
            block.reshape(ent_count, per_owner, width), "ent", 0, 0, tiled=True
        ).reshape(slots, width)

    dma = pltpu.SemaphoreType.DMA
    sent = call(
        export_kernel,
        ((slots, width), BF, ANY),
        [(own, ANY), (export_rows, ANY)],
        scratch=(
            VM((rows, width), BF),
            VM((1, slots), jnp.int32),
            VM((slots, width), BF),
            dma((3,)),
        ),
        flops=LIGHT,
        limit=FULL,
    )
    received = exchange(sent)
    export_next = from_next(export_rows, "tm")
    coef_t = coef.T
    bias_row = gate_bias[None]
    sources = [edge_dst, edge_rel, edge_src, coef_t, rel_emb, basis]
    made = [
        ((blocks * slots, rows), BF),
        ((relations, rows), BF),
        ((rows, LANES), F32),
        ((relations, width), BF),
    ]
    mix, counts, degree_inv, rel_images = call(
        functools.partial(setup_kernel, slots),
        [out + (ANY,) for out in made],
        [(tile_count, pltpu.SMEM)] + [(array, ANY) for array in sources],
        scratch=[VM(array.shape, array.dtype) for array in sources]
        + [VM(dims, kind) for dims, kind in made]
        + [
            VM((edges, rows), BF),
            VM((blocks, edges), F32),
            dma((len(sources),)),
            dma((blocks + 3,)),
        ],
        flops=LIGHT,
        limit=FULL,
    )
    sources = [
        received,
        basis,
        mix,
        self_weight,
        gate_weight,
        bias_row,
        counts,
        rel_images,
        degree_inv,
        own,
        cot,
    ]
    made = [
        ((rows, width), BF),
        ((rows, width), BF),
        ((rows, width), F32),
        ((rows, width), F32),
        ((rows, width), F32),
        ((blocks * slots, width), BF),
    ]
    dense, row_grad, gate, alpha, beta, images = call(
        functools.partial(forward_kernel, slots),
        [out + (ANY,) for out in made],
        [(array, ANY) for array in sources],
        scratch=[VM(array.shape, array.dtype) for array in sources]
        + [VM(dims, kind) for dims, kind in made]
        + [dma((len(sources),)), dma((5, max(rows // 256, 1))), dma],
        flops=LIGHT,
        limit=FULL,
    )

    def slot_step(row_grad):
        return call(
            functools.partial(slot_kernel, slots),
            [((slots, width), BF, VM), ((blocks * slots, width), BF, VM)],
            [(row_grad, VM), (mix, VM), (basis, VM)],
            flops=LIGHT,
        )

    for step in range(1, section_count):
        last = step + 1 == section_count
        slot_grad, _ = slot_step(row_grad)
        ahead = from_next(dense, "tm")
        returned = from_next(exchange(slot_grad), "tm")
        args = [cot, alpha, beta, gate, self_weight, gate_weight]
        args += [ahead, returned, export_next]
        outs = [((rows, width), BF, VM), ((rows, width), F32 if last else BF, VM)]
        if last:
            outs += [((rows, width), BF, VM), ((1, width), F32, VM)]
        outs = call(
            functools.partial(dense_kernel, last),
            outs,
            [(array, VM) for array in args],
            flops=LIGHT,
        )
        row_grad, dense = outs[:2]
    gate_row, bias = outs[2:]

    cut, rel_cut = width // ent_count, relations // ent_count
    first_depth = 3 * cut
    second_depth = (blocks - 1) * cut
    third_depth = rounded_up(rel_cut, 16) + 16
    depth = rounded_up(first_depth + second_depth + third_depth, 16 * section_count)
    distances = []
    while 1 << len(distances) < ent_count:
        distances.append(1 << len(distances))
    orders = (distances, distances[:1] + distances[:0:-1])
    half = ent_count // 2
    kept_a, sent_a, rel_sum = call(
        functools.partial(first_weight_kernel, slots, ent_count, orders[0]),
        [
            ((half, first_depth, width), BF, VM),
            ((half, first_depth, width), BF, VM),
            ((relations, width), F32, VM),
        ],
        [
            (array, VM)
            for array in (
                row_grad,
                gate_row,
                own,
                received,
                mix,
                counts,
                coef_t,
                rel_emb,
            )
        ],
        scratch=[VM((relations, width), BF), VM((width, width), F32)],
        flops=LIGHT,
    )
    slot_grad, mixed = slot_step(row_grad)
    kept_b, sent_b = call(
        functools.partial(second_weight_kernel, slots, ent_count, orders[1]),
        [((half, second_depth, width), BF, VM)] * 2,
        [(array, VM) for array in (received, mixed, coef_t, rel_emb, rel_sum)],
        scratch=[VM((relations, width), BF), VM((width, width), F32)],
        flops=LIGHT,
    )
    packed = call(
        functools.partial(third_weight_kernel, slots, ent_count),
        ((ent_count, per_owner + third_depth, width), BF, VM),
        [(tile_count, pltpu.SMEM)]
        + [
            (array, VM)
            for array in (
                row_grad,
                slot_grad,
                coef_t,
                rel_emb,
                basis,
                bias,
                images,
                rel_sum,
                edge_src,
                edge_dst,
                edge_rel,
            )
        ],
        scratch=[VM((relations, width), BF), VM((256, width), BF)],
        flops=LIGHT,
    )
    packed = lax.all_to_all(packed, "ent", 0, 0, tiled=True)
    folds = [(kept_a, sent_a), (kept_b, sent_b)]
    taken = [None, None]
    for k in range(len(distances)):
        for which in range(2):
            kept, moved = folds[which]
            distance = orders[which][k]
            route = [(i, i ^ distance) for i in range(ent_count)]
            taken[which] = lax.ppermute(moved, "ent", route)
        if k + 1 < len(distances):
            for which in range(2):
                kept = folds[which][0]
                dims = (kept.shape[0] // 2,) + kept.shape[1:]
                folds[which] = call(
                    fold_kernel,
                    [(dims, BF, VM)] * 2,
                    [(kept, VM), (taken[which], VM)],
                    flops=LIGHT,
                )
    joined = call(
        functools.partial(join_kernel, per_owner),
        ((section_count, depth // section_count, width), BF, VM),
        [(folds[0][0], VM), (taken[0], VM), (folds[1][0], VM), (taken[1], VM)]
        + [(packed, VM)],
        flops=LIGHT,
    )
    state_grad = call(
        output_kernel,
        ((rows, width), F32, VM),
        [(dense, VM), (packed, VM), (export_rows, VM)],
        scratch=[VM((slots, width), BF)],
        flops=LIGHT,
    )
    quarter = call(
        quarter_kernel,
        ((depth // section_count, width), BF, VM),
        [(lax.all_to_all(joined, "tm", 0, 0, tiled=True), VM)],
        flops=LIGHT,
    )
    final = lax.all_gather(quarter, "tm", axis=0, tiled=True)
    grad_basis, grad_self, grad_gate, grad_rel, grad_coef, grad_bias = call(
        final_kernel,
        [
            ((cut, blocks * width), F32, VM),
            ((cut, width), F32, VM),
            ((cut, width), F32, VM),
            ((rel_cut, width), F32, VM),
            ((blocks, rel_cut), F32, VM),
            ((1, cut), F32, VM),
        ],
        [(final, VM)],
        flops=LIGHT,
    )
    return (
        state_grad[None],
        grad_basis,
        grad_self,
        grad_gate,
        grad_bias[0],
        grad_coef.T,
        grad_rel,
    )


def solution(mesh):
    placed = (P("tm", "ent", None),) * 2 + (P("tm", "ent"),) * 5 + (P(),) * 6
    return jax.shard_map(
        per_device,
        mesh=mesh,
        in_specs=placed,
        out_specs=(
            P("tm", "ent", None),
            P("ent", None),
            P("ent", None),
            P("ent", None),
            P("ent"),
            P("ent", None),
            P("ent", None),
        ),
        check_vma=False,
    )
```
